512 devices in a mesh: gx: 64 (over y, z), gy: 8 (over x, core).
Axes of the slice: x: 4, y: 8, z: 8, core: 2. Of those that a mesh axis runs over, the one named last changes fastest.
Arguments:
- droplets: float32 [2, 32, 128, 4096], P(None, None, 'gx', 'gy'), as said below
- moves: int32 [2, 32, 128, 4096], P(None, None, 'gx', 'gy'), may hold values from 0 to 8, as said below
- pairing: int32 [2, 32, 128, 4096], P(None, None, 'gx', 'gy'), may hold values from 0 to 31, as said below
- collisions: int32 [2, 16, 128, 4096], P(None, None, 'gx', 'gy'), may hold values from 0 to 3
Outputs:
- droplets_out: float32 [2, 32, 128, 4096], P(None, None, 'gx', 'gy')
- moments: float32 [2, 2, 16], replicated
The draws below stay inside these ranges and needn't reach their ends.
Inputs may be any that keep to these rules, and one draw needn't show every extreme that they name: `droplets`: entry 0 holds whole-number multiplicities from 24 to below 300, entry 1 masses from 0.05 to 2. `moves`: A code c means a step of c // 3 - 1 along x and c % 3 - 1 along y. In each step, slot and level, all droplets of one y-row take the same x-step and all droplets landing in one x-column take the same y-step, so every cell and slot receives exactly one droplet. `pairing`: for each step and cell, the entries along the slot dimension are a permutation of 0 to 31.
All inputs are finite; a program needn't handle non-finite values.
Results may differ from the reference program's by a relative error of at most 0.0003.
Values sent between devices are 32-bit elements; how exact they have to be, the bound alone decides.
A program may use at most 64 MiB of HBM per device.

```python
import jax
import jax.numpy as jnp
from jax import lax

SLOTS = 32
PAIRS = 16
STEPS = 2
LEVELS = 16
NX = 128
NY = 256


def draw_droplets(key, part):
    keys = jax.random.split(jax.random.fold_in(key, 303), 2)
    shape = (SLOTS, NX, NY, LEVELS)
    raw = jax.random.randint(keys[0], shape, 24, 96)
    x_index = lax.broadcasted_iota(jnp.int32, shape, 1)
    counts = (raw * (NX + 2 * x_index) // NX).astype(jnp.float32)
    uniform = jax.random.uniform(keys[1], shape, jnp.float32)
    masses = jnp.exp(jnp.log(0.05) + uniform * (jnp.log(2.0) - jnp.log(0.05)))
    return jnp.stack([counts, masses.astype(jnp.float32)]).reshape(2, SLOTS, NX, NY * LEVELS)


def draw_moves(key, part):
    table = jnp.array([-1, -1, 0, 1, 1], jnp.int32)
    row_key, col_key = jax.random.split(jax.random.fold_in(key, 101))
    shape = (STEPS, SLOTS, NX, NY, LEVELS)
    row_pick = table[jax.random.randint(row_key, (STEPS, SLOTS, 1, NY, LEVELS), 0, 5)]
    col_pick = table[jax.random.randint(col_key, (STEPS, SLOTS, NX, 1, LEVELS), 0, 5)]
    x_index = lax.broadcasted_iota(jnp.int32, shape, 2)
    landing = (x_index + row_pick) % NX
    step_y = jnp.take_along_axis(jnp.broadcast_to(col_pick, shape), landing, axis=2)
    codes = 3 * (row_pick + 1) + step_y + 1
    return codes.reshape(STEPS, SLOTS, NX, NY * LEVELS).astype(jnp.int32)


def draw_pairing(key, part):
    shape = (STEPS, SLOTS, NX, NY * LEVELS)
    scores = jax.random.randint(jax.random.fold_in(key, 202), shape, 0, 1048576) * SLOTS
    scores = scores + lax.broadcasted_iota(jnp.int32, shape, 1)
    return jnp.argsort(scores, axis=1, stable=True).astype(jnp.int32)


def touch_ends(drawn, own_key, least, top_value):
    longest = drawn.shape.index(max(drawn.shape))
    spots = []
    for shift in (0, 1):
        where = [jax.random.randint(jax.random.fold_in(own_key, axis), (), 0, length) for axis, length in enumerate(drawn.shape)]
        where[longest] = (where[longest] + shift) % drawn.shape[longest]
        spots.append(tuple(where))
    return drawn.at[spots[0]].set(least).at[spots[1]].set(top_value)


def setup_inputs(seed: int = 0) -> dict:
    streams_of = jax.random.split(jax.random.key(seed), 5)
    return {
        "droplets": draw_droplets(jax.random.fold_in(streams_of[4], 71), 0),
        "moves": draw_moves(jax.random.fold_in(streams_of[4], 71), 0),
        "pairing": draw_pairing(jax.random.fold_in(streams_of[4], 71), 0),
        "collisions": touch_ends(jax.random.randint(streams_of[3], (STEPS, PAIRS, NX, NY * LEVELS), 0, 4), jax.random.fold_in(streams_of[3], 1), 0, 3).astype(jnp.int32),
    }


count_unit = 4096.0


def migrate(state, codes):
    moved = jnp.zeros_like(state)
    for direction in range(9):
        step_x = direction // 3 - 1
        step_y = direction % 3 - 1
        chosen = jnp.where((codes == direction)[None], state, jnp.zeros_like(state))
        moved = moved + jnp.roll(chosen, (step_x, step_y), axis=(2, 3))
    return moved


def collide(first_count, second_count, first_mass, second_mass, tries):
    big_first = first_count >= second_count
    larger = jnp.where(big_first, first_count, second_count)
    smaller = jnp.where(big_first, second_count, first_count)
    larger_mass = jnp.where(big_first, first_mass, second_mass)
    smaller_mass = jnp.where(big_first, second_mass, first_mass)
    taken = jnp.minimum(tries, larger // smaller)
    remain = larger - taken * smaller
    splits = remain == 0
    halved = smaller // 2
    larger_new = jnp.where(splits, halved, remain)
    smaller_new = jnp.where(splits, smaller - halved, smaller)
    grown = smaller_mass + taken.astype(first_mass.dtype) * larger_mass
    larger_mass_new = jnp.where(splits, grown, larger_mass)
    first_new = jnp.where(big_first, larger_new, smaller_new)
    second_new = jnp.where(big_first, smaller_new, larger_new)
    first_mass_new = jnp.where(big_first, larger_mass_new, grown)
    second_mass_new = jnp.where(big_first, grown, larger_mass_new)
    return first_new, second_new, first_mass_new, second_mass_new


def coalesce(state, order, tries):
    counts = state[0].astype(jnp.int32)
    masses = state[1]
    counts_p = jnp.take_along_axis(counts, order, axis=0)
    masses_p = jnp.take_along_axis(masses, order, axis=0)
    first_new, second_new, first_mass, second_mass = collide(counts_p[0::2], counts_p[1::2], masses_p[0::2], masses_p[1::2], tries)
    counts_pair = jnp.stack([first_new, second_new], axis=1).reshape(counts_p.shape)
    masses_pair = jnp.stack([first_mass, second_mass], axis=1).reshape(masses_p.shape)
    inverse = jnp.argsort(order, axis=0).astype(jnp.int32)
    counts_new = jnp.take_along_axis(counts_pair, inverse, axis=0)
    masses_new = jnp.take_along_axis(masses_pair, inverse, axis=0)
    return jnp.stack([counts_new.astype(state.dtype), masses_new])


def level_moments(state):
    count_sum = jnp.sum(state[0], axis=(0, 1, 2))
    liquid_sum = jnp.sum(state[0] * state[1], axis=(0, 1, 2))
    return jnp.stack([count_sum, liquid_sum]) / (NX * NY * count_unit)


def reference(droplets, moves, pairing, collisions):
    state = droplets.reshape(2, SLOTS, NX, NY, LEVELS)
    codes = moves.reshape(STEPS, SLOTS, NX, NY, LEVELS)
    orders = pairing.reshape(STEPS, SLOTS, NX, NY, LEVELS)
    tries = collisions.reshape(STEPS, PAIRS, NX, NY, LEVELS)
    results = []
    for step in range(STEPS):
        state = migrate(state, codes[step])
        state = coalesce(state, orders[step], tries[step])
        results.append(level_moments(state))
    return state.reshape(droplets.shape), jnp.stack(results)
```

```python
import jax
import jax.numpy as jnp
from jax import lax
from jax.experimental import pallas as pl
from jax.experimental.pallas import tpu as pltpu
from jax.sharding import PartitionSpec as P

MESH = pl.DeviceIdType.MESH
SLOTS = 32
LEVELS = 16
GROUPS = 4
CHUNKS = 4
STEPS = 2
Z_RING = 8
count_unit = 4096.0


def row0(base, slot, chunk, col):
    return ((base * SLOTS + slot) * CHUNKS + chunk) * 2 + col


def rows_of(ref, base, group, chunk, col):
    return ref[pl.ds(row0(base, 8 * group, chunk, col), 8, stride=8), :]


def roll(x, shift):
    return pltpu.roll(x, shift % 128, axis=x.ndim - 1)


def make_kernel(nx, ny, z_ring):
    y_ring = nx // z_ring
    rings = (ny, y_ring, z_ring)
    peers = sum(r - 1 for r in rings) + 8
    scale = 1.0 / (nx * 2 * ny * 32 * count_unit)

    def kernel(drop, mov, pair, coll, out, mom, d_in, m_in, p_in, c_in, st, fs, fr, own, rs, rr, code, coef, o_buf, ar,
               in_sem, f_send, f_recv, r_send, r_recv, a_send, a_recv, o_sem):
        gx = lax.axis_index("gx")
        gy = lax.axis_index("gy")
        loads = [
            pltpu.make_async_copy(src, dst, in_sem.at[i])
            for i, (src, dst) in enumerate(((drop, d_in), (mov, m_in), (pair, p_in), (coll, c_in)))
        ]
        for load in loads:
            load.start()

        def at(dx, dy):
            return (lax.rem(gx + dx + nx, nx), lax.rem(gy + dy + ny, ny))

        y_pos = gx // z_ring
        z_pos = lax.rem(gx, z_ring)
        places = (gy, y_pos, z_pos)

        def peer(stage, other):
            if stage == 0:
                return (gx, other)
            if stage == 1:
                return (other * z_ring + z_pos, gy)
            return (y_pos * z_ring + other, gy)

        barrier = pltpu.get_barrier_semaphore()
        for dx in (-1, 0, 1):
            for dy in (-1, 0, 1):
                if dx or dy:
                    pl.semaphore_signal(barrier, inc=1, device_id=at(dx, dy), device_id_type=MESH)
        for stage in range(3):
            for d in range(1, rings[stage]):
                other = lax.rem(places[stage] + d, rings[stage])
                pl.semaphore_signal(barrier, inc=1, device_id=peer(stage, other), device_id_type=MESH)

        lane = lax.broadcasted_iota(jnp.int32, (8, 128), 1)
        lane4 = lax.broadcasted_iota(jnp.int32, (CHUNKS, 8, 128), 2)
        first_row = lane4 < LEVELS
        last_row = lane4 >= 128 - LEVELS
        zero = jnp.zeros((8, 128), jnp.float32)
        copies = []

        def value(step, nm, col, group):
            if step == 0:
                return jnp.stack([rows_of(d_in, nm, group, k, col) for k in range(CHUNKS)])
            return st[nm, col, :, 8 * group : 8 * group + 8, :]

        def codes(step, col, group):
            return jnp.stack([rows_of(m_in, step, group, k, col) for k in range(CHUNKS)])

        def place(down, stay, up):
            up_r = roll(up, LEVELS)
            up_s = jnp.where(first_row, jnp.concatenate([zero[None], up_r[:-1]]), up_r)
            down_r = roll(down, -LEVELS)
            down_s = jnp.where(last_row, jnp.concatenate([down_r[1:], zero[None]]), down_r)
            return stay + up_s + down_s

        def piece(x, k):
            return jnp.where((lane >> 4) == k, x, zero)

        def remote(src, dst, send, recv, target):
            copy = pltpu.make_async_remote_copy(src, dst, send, recv, device_id=target, device_id_type=MESH)
            copy.start()
            copies.append(copy)

        def send_faces(step, nm):
            up_rim = zero
            down_rim = zero
            for g in range(GROUPS):
                for side in range(2):
                    col = 1 - side
                    first = 6 if side == 0 else 0
                    x = value(step, nm, col, g)
                    c = codes(step, col, g)
                    none = jnp.zeros_like(x)
                    down = jnp.where(c == first, x, none)
                    stay = jnp.where(c == first + 1, x, none)
                    up = jnp.where(c == first + 2, x, none)
                    fs[step, nm, side, :, 8 * g : 8 * g + 8, :] = place(down, stay, up)
                    k = side * GROUPS + g
                    up_rim = up_rim + piece(roll(up[CHUNKS - 1], 16 * k + 16), k)
                    down_rim = down_rim + piece(roll(down[0], 16 * k), k)
            rs[step, nm, 2] = up_rim
            rs[step, nm, 3] = down_rim
            for side in range(2):
                remote(fs.at[step, nm, side], fr.at[step, nm, side], f_send.at[step, nm, side], f_recv.at[step, nm, side],
                       at(1 - 2 * side, 0))
            for i in range(4):
                side, down = i // 2, i % 2
                remote(rs.at[step, nm, 2 + down], rr.at[step, nm, 2 + i], r_send.at[step, nm, 2 + i],
                       r_recv.at[step, nm, 2 + i], at(1 - 2 * side, 1 - 2 * down))

        def send_rims(step, nm):
            up_rim = zero
            down_rim = zero
            for g in range(GROUPS):
                x0 = value(step, nm, 0, g)
                x1 = value(step, nm, 1, g)
                c0 = codes(step, 0, g)
                c1 = codes(step, 1, g)
                none = jnp.zeros_like(x0)
                for col in range(2):
                    a = 3 + 3 * col
                    b = 3 * col
                    down = jnp.where(c0 == a, x0, jnp.where(c1 == b, x1, none))
                    stay = jnp.where(c0 == a + 1, x0, jnp.where(c1 == b + 1, x1, none))
                    up = jnp.where(c0 == a + 2, x0, jnp.where(c1 == b + 2, x1, none))
                    own[nm, col, :, 8 * g : 8 * g + 8, :] = place(down, stay, up)
                    k = col * GROUPS + g
                    up_rim = up_rim + piece(roll(up[CHUNKS - 1], 16 * k + 16), k)
                    down_rim = down_rim + piece(roll(down[0], 16 * k), k)
            rs[step, nm, 0] = up_rim
            rs[step, nm, 1] = down_rim
            for down in range(2):
                remote(rs.at[step, nm, down], rr.at[step, nm, down], r_send.at[step, nm, down], r_recv.at[step, nm, down],
                       at(0, 1 - 2 * down))

        def arrived(step, nm):
            for side in range(2):
                f = fs.at[step, nm, side]
                pltpu.make_async_remote_copy(f, fr.at[step, nm, side], f_send.at[step, nm, side], f_recv.at[step, nm, side],
                                             device_id=at(1 - 2 * side, 0), device_id_type=MESH).wait_recv()
            for i in range(6):
                pltpu.make_async_remote_copy(rs.at[step, nm, 0], rr.at[step, nm, i], r_send.at[step, nm, i],
                                             r_recv.at[step, nm, i], device_id=at(0, 1), device_id_type=MESH).wait_recv()
            low = rr[step, nm, 0] + jnp.where(lane < 64, rr[step, nm, 2], rr[step, nm, 4])
            high = rr[step, nm, 1] + jnp.where(lane < 64, rr[step, nm, 3], rr[step, nm, 5])
            return low, high

        def joined(step, nm, col, k, low, high):
            parts = []
            for g in range(GROUPS):
                x = own[nm, col, k, 8 * g : 8 * g + 8, :] + fr[step, nm, col, k, 8 * g : 8 * g + 8, :]
                j = 16 * (col * GROUPS + g)
                if k == 0:
                    x = x + jnp.where(lane < LEVELS, roll(low, -j), zero)
                if k == CHUNKS - 1:
                    x = x + jnp.where(lane >= 128 - LEVELS, roll(high, 112 - j), zero)
                parts.append(x)
            return parts

        def partner_of(parts, c):
            low = c & 7
            high = (c >> 3) & 3
            got = jnp.take_along_axis(parts[0], low, axis=0, mode="promise_in_bounds")
            for g in range(1, GROUPS):
                got = jnp.where(high == g, jnp.take_along_axis(parts[g], low, axis=0, mode="promise_in_bounds"), got)
            return got

        def pair_codes(step):
            def body(i, carry):
                col = i % 2
                k = i // 2
                slot = [lax.broadcasted_iota(jnp.int32, (8, 128), 0) + 8 * g for g in range(GROUPS)]
                acc = [jnp.zeros((8, 128), jnp.int32) for g in range(GROUPS)]
                for p in range(SLOTS // 2):
                    a = jnp.broadcast_to(p_in[pl.ds(row0(step, 2 * p, k, col), 1), :], (8, 128))
                    b = jnp.broadcast_to(p_in[pl.ds(row0(step, 2 * p + 1, k, col), 1), :], (8, 128))
                    g0 = jnp.broadcast_to(c_in[pl.ds(((step * 16 + p) * CHUNKS + k) * 2 + col, 1), :], (8, 128)) * 32
                    for_a = b + g0 + 128
                    for_b = a + g0
                    for g in range(GROUPS):
                        acc[g] = jnp.where(a == slot[g], for_a, jnp.where(b == slot[g], for_b, acc[g]))
                for g in range(GROUPS):
                    code[step, col, k, 8 * g : 8 * g + 8, :] = acc[g]
                return carry

            lax.fori_loop(0, 2 * CHUNKS, body, 0)

        def out_rows(nm, g, k, col, x):
            o_buf[pl.ds(row0(nm, 8 * g, k, col), 8, stride=8), :] = x

        def coalesce_n(step):
            low, high = arrived(step, 0)
            total = zero
            for col in range(2):
                for k in range(CHUNKS):
                    parts = joined(step, 0, col, k, low, high)
                    for g in range(GROUPS):
                        c = code[step, col, k, 8 * g : 8 * g + 8, :]
                        mine = parts[g]
                        other = partner_of(parts, c)
                        g0 = ((c >> 5) & 3).astype(jnp.float32)
                        ahead = jnp.where(c >= 128, 0.5, 0.0)
                        big = jnp.maximum(mine, other)
                        small = jnp.minimum(mine, other)
                        mine_big = mine + ahead > other
                        fits = jnp.where(small * 3.0 <= big, 3.0, jnp.where(small * 2.0 <= big, 2.0, 1.0))
                        taken = jnp.minimum(g0, fits)
                        rest = big - taken * small
                        splits = rest == 0.0
                        half = jnp.floor(small * 0.5)
                        new = jnp.where(mine_big, jnp.where(splits, half, rest), jnp.where(splits, small - half, small))
                        keep = jnp.where(mine_big, jnp.where(splits, taken, 1.0), 1.0)
                        add = jnp.where(mine_big, jnp.where(splits, 1.0, 0.0), taken)
                        coef[0, col, k, 8 * g : 8 * g + 8, :] = keep
                        coef[1, col, k, 8 * g : 8 * g + 8, :] = add
                        st[0, col, k, 8 * g : 8 * g + 8, :] = new
                        total = total + new
                        if step == STEPS - 1:
                            out_rows(0, g, k, col, new)
            return total

        def coalesce_m(step):
            low, high = arrived(step, 1)
            total = zero
            for col in range(2):
                for k in range(CHUNKS):
                    parts = joined(step, 1, col, k, low, high)
                    for g in range(GROUPS):
                        c = code[step, col, k, 8 * g : 8 * g + 8, :]
                        other = partner_of(parts, c)
                        new = coef[0, col, k, 8 * g : 8 * g + 8, :] * parts[g] + coef[1, col, k, 8 * g : 8 * g + 8, :] * other
                        if step < STEPS - 1:
                            st[1, col, k, 8 * g : 8 * g + 8, :] = new
                        else:
                            out_rows(1, g, k, col, new)
                        total = total + st[0, col, k, 8 * g : 8 * g + 8, :] * new
            return total

        loads[0].wait()
        loads[1].wait()
        pl.semaphore_wait(barrier, peers)
        sums = []
        outs = []
        for step in range(STEPS):
            if step == 0:
                send_faces(step, 0)
                send_rims(step, 0)
                send_faces(step, 1)
                send_rims(step, 1)
                loads[2].wait()
                loads[3].wait()
                pair_codes(0)
                pair_codes(1)
            count = coalesce_n(step)
            if step < STEPS - 1:
                send_faces(step + 1, 0)
                send_rims(step + 1, 0)
            else:
                outs.append(pltpu.make_async_copy(o_buf.at[pl.ds(0, 256)], out.at[pl.ds(0, 256)], o_sem.at[0]))
                outs[-1].start()
            liquid = coalesce_m(step)
            if step < STEPS - 1:
                send_faces(step + 1, 1)
                send_rims(step + 1, 1)
            else:
                outs.append(pltpu.make_async_copy(o_buf.at[pl.ds(256, 256)], out.at[pl.ds(256, 256)], o_sem.at[1]))
                outs[-1].start()
            sums.append(jnp.sum(count, axis=0, keepdims=True))
            sums.append(jnp.sum(liquid, axis=0, keepdims=True))
        total = jnp.concatenate(sums, axis=0)
        for stage in range(3):
            place_of = places[stage]
            ar[stage, place_of] = total
            for d in range(1, rings[stage]):
                other = lax.rem(place_of + d, rings[stage])
                remote(ar.at[stage, place_of], ar.at[stage, place_of], a_send.at[stage, d], a_recv.at[stage, place_of],
                       peer(stage, other))
            for d in range(1, rings[stage]):
                other = lax.rem(place_of + d, rings[stage])
                pltpu.make_async_remote_copy(ar.at[stage, other], ar.at[stage, other], a_send.at[stage, d],
                                             a_recv.at[stage, other], device_id=peer(stage, other),
                                             device_id_type=MESH).wait_recv()
            total = ar[stage, 0]
            for d in range(1, rings[stage]):
                total = total + ar[stage, d]
        folded = total
        for d in range(1, 8):
            folded = folded + roll(total, LEVELS * d)
        folded = folded * scale
        for step in range(STEPS):
            mom[step] = folded[2 * step : 2 * step + 2, :LEVELS]
        for copy in copies:
            copy.wait_send()
        for copy in outs:
            copy.wait()

    return kernel


def shards(nx, ny, z_ring):
    def rows(x):
        a, b, cols, flat = x.shape
        x = x.reshape(a, b, cols, CHUNKS, 128).transpose(0, 1, 3, 2, 4)
        return x.reshape(a * b * CHUNKS * cols, 128)

    def step(droplets, moves, pairing, collisions):
        f32 = jnp.float32
        i32 = jnp.int32
        dma = pltpu.SemaphoreType.DMA
        ring = max(ny, nx // z_ring, z_ring)
        hbm = pl.BlockSpec(memory_space=pl.ANY)
        vmem = pl.BlockSpec(memory_space=pltpu.VMEM)
        out, mom = pl.pallas_call(
            make_kernel(nx, ny, z_ring),
            out_shape=(jax.ShapeDtypeStruct((512, 128), f32), jax.ShapeDtypeStruct((STEPS, 2, LEVELS), f32)),
            in_specs=[hbm] * 4,
            out_specs=(hbm, vmem),
            scratch_shapes=[
                pltpu.VMEM((512, 128), f32),
                pltpu.VMEM((512, 128), i32),
                pltpu.VMEM((512, 128), i32),
                pltpu.VMEM((256, 128), i32),
                pltpu.VMEM((2, 2, CHUNKS, SLOTS, 128), f32),
                pltpu.VMEM((STEPS, 2, 2, CHUNKS, SLOTS, 128), f32),
                pltpu.VMEM((STEPS, 2, 2, CHUNKS, SLOTS, 128), f32),
                pltpu.VMEM((2, 2, CHUNKS, SLOTS, 128), f32),
                pltpu.VMEM((STEPS, 2, 4, 8, 128), f32),
                pltpu.VMEM((STEPS, 2, 6, 8, 128), f32),
                pltpu.VMEM((STEPS, 2, CHUNKS, SLOTS, 128), i32),
                pltpu.VMEM((2, 2, CHUNKS, SLOTS, 128), f32),
                pltpu.VMEM((512, 128), f32),
                pltpu.VMEM((3, ring, 4, 128), f32),
                dma((4,)),
                dma((STEPS, 2, 2)),
                dma((STEPS, 2, 2)),
                dma((STEPS, 2, 6)),
                dma((STEPS, 2, 6)),
                dma((3, ring)),
                dma((3, ring)),
                dma((2,)),
            ],
            compiler_params=pltpu.CompilerParams(collective_id=0, has_side_effects=True),
        )(rows(droplets), rows(moves), rows(pairing), rows(collisions))
        out = out.reshape(2, SLOTS, CHUNKS, 2, 128).transpose(0, 1, 3, 2, 4).reshape(droplets.shape)
        return out, mom

    return step


def solution(mesh, z_ring=Z_RING):
    placed = P(None, None, "gx", "gy")
    return jax.shard_map(
        shards(mesh.shape["gx"], mesh.shape["gy"], z_ring), mesh=mesh, in_specs=(placed,) * 4, out_specs=(placed, P()),
        check_vma=False,
    )
```

```python
import jax
import jax.numpy as jnp
from jax import lax
from jax.experimental import pallas as pl
from jax.experimental.pallas import tpu as pltpu
from jax.sharding import PartitionSpec as P

MESH = pl.DeviceIdType.MESH
SLOTS = 32
PAIRS = 16
LEVELS = 16
GROUPS = 4
CHUNKS = 4
STEPS = 2
Z_RING = 8
count_unit = 4096.0


def row0(base, slot, chunk, col):
    return ((base * SLOTS + slot) * CHUNKS + chunk) * 2 + col


def eight(base, group, chunk, col):
    return pl.ds(row0(base, 8 * group, chunk, col), 8, stride=8)


def roll(x, shift):
    return pltpu.roll(x, shift % 128, axis=x.ndim - 1)


def wrapped(i, d, size):
    j = i + d
    if d > 0:
        return jnp.where(j >= size, j - size, j)
    return jnp.where(j < 0, j + size, j)


def tree_sum(terms):
    while len(terms) > 1:
        terms = [a + b for a, b in zip(terms[::2], terms[1::2])] + ([terms[-1]] if len(terms) % 2 else [])
    return terms[0]


def doublings(size):
    return [1 << i for i in range(10) if (1 << i) < size // 2]


def make_kernel(nx, ny, z_ring):
    y_ring = nx // z_ring
    rounds = [("x", d) for d in doublings(nx)] + [("y", d) for d in doublings(ny)]
    scale = 1.0 / (nx * 2 * ny * 32 * count_unit)

    def hops(d):
        dy, dz = d // z_ring, d % z_ring
        return min(dy, y_ring - dy) + min(dz, z_ring - dz)

    far_first = sorted(range(1, nx), key=lambda d: -hops(d))

    def kernel(drop, mov, pair, coll, out, mom, d_in, m_in, p_in, c_in, st, fs, fr, own, rs, rr, code, coef, ar_y, ar_x,
               in_sem, f_send, f_recv, r_send, r_recv, a_send, a_recv, known):
        gx = lax.axis_index("gx")
        gy = lax.axis_index("gy")
        halves = lambda src, dst, i, n: (src.at[pl.ds(i * n, n)], dst.at[pl.ds(i * n, n)])
        n_load, move_load, m_load, pair_load, coll_load, later_load = [
            pltpu.make_async_copy(src, dst, in_sem.at[i])
            for i, (src, dst) in enumerate(
                (
                    halves(drop, d_in, 0, 256),
                    halves(mov, m_in, 0, 256),
                    halves(drop, d_in, 1, 256),
                    (pair, p_in),
                    (coll, c_in),
                    halves(mov, m_in, 1, 256),
                )
            )
        ]
        n_load.start()
        move_load.start()
        xs = {0: gx, 1: wrapped(gx, 1, nx), -1: wrapped(gx, -1, nx)}
        ys = {0: gy, 1: wrapped(gy, 1, ny), -1: wrapped(gy, -1, ny)}
        barrier = pltpu.get_barrier_semaphore()
        for dx in (-1, 1, 0):
            for dy in (-1, 0, 1):
                if dx or dy:
                    pl.semaphore_signal(barrier, inc=1, device_id=(xs[dx], ys[dy]), device_id_type=MESH)
        m_load.start()
        pair_load.start()
        coll_load.start()
        later_load.start()

        lane = lax.broadcasted_iota(jnp.int32, (8, 128), 1)
        first_row = lane < LEVELS
        last_row = lane >= 128 - LEVELS
        zero = jnp.zeros((8, 128), jnp.float32)
        copies = []

        def tell(i):
            axis, d = rounds[i]
            for e in (d, -d):
                target = (wrapped(gx, e, nx), gy) if axis == "x" else (gx, wrapped(gy, e, ny))
                pl.semaphore_signal(known.at[i], inc=1, device_id=target, device_id_type=MESH)

        def hear(i):
            pl.semaphore_wait(known.at[i], 2)

        def value(step, nm, col, k, g):
            if step == 0:
                return d_in[eight(nm, g, k, col), :]
            return st[nm, col, k, 8 * g : 8 * g + 8, :]

        def moves(step, col, k, g):
            return m_in[eight(step, g, k, col), :]

        def leaving(step, nm, side, k, g):
            x = value(step, nm, 1 - side, k, g)
            c = moves(step, 1 - side, k, g)
            first = 6 if side == 0 else 0
            return [jnp.where(c == first + i, x, zero) for i in range(3)]

        def staying(step, nm, col, k, g):
            x0 = value(step, nm, 0, k, g)
            x1 = value(step, nm, 1, k, g)
            c0 = moves(step, 0, k, g)
            c1 = moves(step, 1, k, g)
            a = 3 + 3 * col
            b = 3 * col
            return [jnp.where(c0 == a + i, x0, jnp.where(c1 == b + i, x1, zero)) for i in range(3)]

        def remote(src, dst, send, recv, target):
            copy = pltpu.make_async_remote_copy(src, dst, send, recv, device_id=target, device_id_type=MESH)
            copy.start()
            copies.append(copy)

        def send_rims(step, nm):
            for kind, part in enumerate((staying, leaving)):
                ups = []
                downs = []
                for i in range(2):
                    for g in range(GROUPS):
                        j = 16 * (i * GROUPS + g)
                        mine = (lane >= j) & (lane < j + 16)
                        ups.append(jnp.where(mine, roll(part(step, nm, i, CHUNKS - 1, g)[2], j + 16), zero))
                        downs.append(jnp.where(mine, roll(part(step, nm, i, 0, g)[0], j), zero))
                rs[step, nm, 2 * kind] = tree_sum(ups)
                rs[step, nm, 2 * kind + 1] = tree_sum(downs)
            for i in range(6):
                side, down = i // 2 - 1, i % 2
                target = (xs[0 if i < 2 else 1 - 2 * side], ys[1 - 2 * down])
                remote(rs.at[step, nm, down + (2 if i >= 2 else 0)], rr.at[step, nm, i], r_send.at[step, nm, i],
                       r_recv.at[step, nm, i], target)

        def send_chunk(step, nm, k):
            for side in range(2):
                remote(fs.at[step, nm, side, k], fr.at[step, nm, side, k], f_send.at[step, nm, side, k],
                       f_recv.at[step, nm, side, k], (xs[1 - 2 * side], gy))

        def send_faces(step, nm, k, held):
            now = {}
            for side in range(2):
                for g in range(GROUPS):
                    down, stay, up = leaving(step, nm, side, k, g)
                    up = roll(up, LEVELS)
                    down = roll(down, -LEVELS)
                    before = zero
                    if k > 0:
                        face, before = held[side, g]
                        fs[step, nm, side, k - 1, 8 * g : 8 * g + 8, :] = face + jnp.where(last_row, down, zero)
                    face = stay + jnp.where(first_row, before, up) + jnp.where(last_row, zero, down)
                    if k == CHUNKS - 1:
                        fs[step, nm, side, k, 8 * g : 8 * g + 8, :] = face
                    now[side, g] = (face, up)
            if k > 0:
                send_chunk(step, nm, k - 1)
            if k == CHUNKS - 1:
                send_chunk(step, nm, k)
            return now

        def keep_own(step, nm):
            for col in range(2):
                for g in range(GROUPS):
                    downs, stays, ups = zip(*[staying(step, nm, col, k, g) for k in range(CHUNKS)])
                    ups = [zero] + [roll(x, LEVELS) for x in ups]
                    downs = [roll(x, -LEVELS) for x in downs] + [zero]
                    for k in range(CHUNKS):
                        own[step, nm, col, k, 8 * g : 8 * g + 8, :] = (
                            stays[k] + jnp.where(first_row, ups[k], ups[k + 1]) + jnp.where(last_row, downs[k + 1], downs[k])
                        )

        def wait_rims(step, nm):
            for i in range(6):
                pltpu.make_async_remote_copy(rs.at[step, nm, 0], rr.at[step, nm, i], r_send.at[step, nm, i],
                                             r_recv.at[step, nm, i], device_id=(gx, ys[1]), device_id_type=MESH).wait_recv()
            low = rr[step, nm, 0] + jnp.where(lane < 64, rr[step, nm, 2], rr[step, nm, 4])
            high = rr[step, nm, 1] + jnp.where(lane < 64, rr[step, nm, 3], rr[step, nm, 5])
            return low, high

        def wait_chunk(step, nm, k):
            for side in range(2):
                pltpu.make_async_remote_copy(fs.at[step, nm, side, k], fr.at[step, nm, side, k], f_send.at[step, nm, side, k],
                                             f_recv.at[step, nm, side, k], device_id=(xs[1], gy),
                                             device_id_type=MESH).wait_recv()

        def joined(step, nm, col, k, rims):
            parts = []
            for g in range(GROUPS):
                x = own[step, nm, col, k, 8 * g : 8 * g + 8, :] + fr[step, nm, col, k, 8 * g : 8 * g + 8, :]
                j = 16 * (col * GROUPS + g)
                if k == 0:
                    x = x + jnp.where(first_row, roll(rims[0], -j), zero)
                if k == CHUNKS - 1:
                    x = x + jnp.where(last_row, roll(rims[1], 112 - j), zero)
                parts.append(x)
            return parts

        def partner_of(parts, c):
            low = c & 7
            high = (c >> 3) & 3
            got = jnp.take_along_axis(parts[0], low, axis=0, mode="promise_in_bounds")
            for g in range(1, GROUPS):
                got = jnp.where(high == g, jnp.take_along_axis(parts[g], low, axis=0, mode="promise_in_bounds"), got)
            return got

        def pair_codes(step):
            def body(i, carry):
                col = i % 2
                k = i // 2
                slot = [lax.broadcasted_iota(jnp.int32, (8, 128), 0) + 8 * g for g in range(GROUPS)]
                acc = [jnp.zeros((8, 128), jnp.int32) for g in range(GROUPS)]
                for p in range(PAIRS):
                    a = jnp.broadcast_to(p_in[pl.ds(row0(step, 2 * p, k, col), 1), :], (8, 128))
                    b = jnp.broadcast_to(p_in[pl.ds(row0(step, 2 * p + 1, k, col), 1), :], (8, 128))
                    g0 = jnp.broadcast_to(c_in[pl.ds(((step * PAIRS + p) * CHUNKS + k) * 2 + col, 1), :], (8, 128)) * 32
                    for_a = b + g0 + 128
                    for_b = a + g0
                    for g in range(GROUPS):
                        acc[g] = jnp.where(a == slot[g], for_a, jnp.where(b == slot[g], for_b, acc[g]))
                for g in range(GROUPS):
                    code[step, col, k, 8 * g : 8 * g + 8, :] = acc[g]
                return carry

            lax.fori_loop(0, 2 * CHUNKS, body, 0)

        def coalesce_n(step, k, rims):
            total = []
            for col in range(2):
                parts = joined(step, 0, col, k, rims)
                for g in range(GROUPS):
                    c = code[step, col, k, 8 * g : 8 * g + 8, :]
                    mine = parts[g]
                    other = partner_of(parts, c)
                    g0 = ((c >> 5) & 3).astype(jnp.float32)
                    ahead = jnp.where(c >= 128, 0.5, 0.0)
                    big = jnp.maximum(mine, other)
                    small = jnp.minimum(mine, other)
                    mine_big = mine + ahead > other
                    fits = jnp.where(small * 3.0 <= big, 3.0, jnp.where(small * 2.0 <= big, 2.0, 1.0))
                    taken = jnp.minimum(g0, fits)
                    rest = big - taken * small
                    splits = rest == 0.0
                    half = jnp.floor(small * 0.5)
                    new = jnp.where(mine_big, jnp.where(splits, half, rest), jnp.where(splits, small - half, small))
                    coef[0, col, k, 8 * g : 8 * g + 8, :] = jnp.where(mine_big, jnp.where(splits, taken, 1.0), 1.0)
                    coef[1, col, k, 8 * g : 8 * g + 8, :] = jnp.where(mine_big, jnp.where(splits, 1.0, 0.0), taken)
                    st[0, col, k, 8 * g : 8 * g + 8, :] = new
                    total.append(new)
                    if step == STEPS - 1:
                        out[eight(0, g, k, col), :] = new
            return tree_sum(total)

        def coalesce_m(step, k, rims):
            total = []
            for col in range(2):
                parts = joined(step, 1, col, k, rims)
                for g in range(GROUPS):
                    c = code[step, col, k, 8 * g : 8 * g + 8, :]
                    other = partner_of(parts, c)
                    new = coef[0, col, k, 8 * g : 8 * g + 8, :] * parts[g] + coef[1, col, k, 8 * g : 8 * g + 8, :] * other
                    if step < STEPS - 1:
                        st[1, col, k, 8 * g : 8 * g + 8, :] = new
                    else:
                        out[eight(1, g, k, col), :] = new
                    total.append(st[0, col, k, 8 * g : 8 * g + 8, :] * new)
            return tree_sum(total)

        def level_row(step, count, liquid, row):
            both = jnp.concatenate([jnp.sum(count, axis=0, keepdims=True), jnp.sum(liquid, axis=0, keepdims=True)], axis=0)
            both = tree_sum([both] + [roll(both, LEVELS * d) for d in range(1, 128 // LEVELS)])
            slot = lane[:1] >> 4
            return jnp.where(slot == 2 * step, both[:1], jnp.where(slot == 2 * step + 1, both[1:], row))

        def both_axes(i):
            n = len(doublings(nx))
            return ([i] if i < n else []) + ([n + i] if n + i < len(rounds) else [])

        def tell_both(i):
            for j in both_axes(i):
                tell(j)

        def hear_both(i):
            for j in both_axes(i):
                hear(j)

        with jax.named_scope("load"):
            n_load.wait()
            move_load.wait()
        with jax.named_scope("barrier"):
            pl.semaphore_wait(barrier, 8)
        with jax.named_scope("send_n"):
            held = send_faces(0, 0, 0, None)
            held = send_faces(0, 0, 1, held)
            send_rims(0, 0)
            held = send_faces(0, 0, 2, held)
            send_faces(0, 0, 3, held)
        with jax.named_scope("send_m"):
            m_load.wait()
            held = send_faces(0, 1, 0, None)
            held = send_faces(0, 1, 1, held)
            send_rims(0, 1)
            held = send_faces(0, 1, 2, held)
            send_faces(0, 1, 3, held)
        with jax.named_scope("own"):
            tell_both(0)
            keep_own(0, 0)
            keep_own(0, 1)
        with jax.named_scope("codes"):
            pair_load.wait()
            coll_load.wait()
            later_load.wait()
            pair_codes(0)
        with jax.named_scope("round"):
            hear_both(0)
            tell_both(1)
        counts = []
        liquids = []
        with jax.named_scope("wait_n"):
            rims = wait_rims(0, 0)
        for k in range(CHUNKS):
            with jax.named_scope("wait_n"):
                wait_chunk(0, 0, k)
            with jax.named_scope("step_n"):
                counts.append(coalesce_n(0, k, rims))
                held = send_faces(1, 0, k, held)
        with jax.named_scope("rims_n"):
            send_rims(1, 0)
        with jax.named_scope("wait_m"):
            rims = wait_rims(0, 1)
        for k in range(CHUNKS):
            with jax.named_scope("wait_m"):
                wait_chunk(0, 1, k)
            with jax.named_scope("step_m"):
                liquids.append(coalesce_m(0, k, rims))
                held = send_faces(1, 1, k, held)
        with jax.named_scope("rims_m"):
            send_rims(1, 1)
        with jax.named_scope("round"):
            hear_both(1)
            tell_both(2)
        with jax.named_scope("own"):
            keep_own(1, 0)
            keep_own(1, 1)
        with jax.named_scope("codes"):
            pair_codes(1)
            row = level_row(0, tree_sum(counts), tree_sum(liquids), jnp.zeros((1, 128), jnp.float32))
        with jax.named_scope("wait_n"):
            rims = wait_rims(1, 0)
            for k in range(CHUNKS):
                wait_chunk(1, 0, k)
        with jax.named_scope("coalesce_n"):
            count = tree_sum([coalesce_n(1, k, rims) for k in range(CHUNKS)])
        with jax.named_scope("round"):
            hear_both(2)
            tell_both(3)
        with jax.named_scope("wait_m"):
            rims = wait_rims(1, 1)
            for k in range(CHUNKS):
                wait_chunk(1, 1, k)
        with jax.named_scope("coalesce_m"):
            liquid = tree_sum([coalesce_m(1, k, rims) for k in range(CHUNKS)])
            row = level_row(1, count, liquid, row)

        def all_send(buf, sem, n):
            return pltpu.make_async_remote_copy(buf.at[pl.ds(0, n)], buf.at[pl.ds(0, n)], a_send.at[sem], a_recv.at[sem],
                                                device_id=(gx, ys[1]), device_id_type=MESH)

        with jax.named_scope("reduce_y"):
            ar_y[gy] = row
            for d in range(1, ny):
                pltpu.make_async_remote_copy(ar_y.at[gy], ar_y.at[gy], a_send.at[0], a_recv.at[0],
                                             device_id=(gx, wrapped(gy, d, ny)), device_id_type=MESH).start()
            for i in range(3, max(len(doublings(nx)), 4)):
                hear_both(i)
                tell_both(i + 1)
            all_send(ar_y, 0, ny - 1).wait_recv()
            row = tree_sum([ar_y[i] for i in range(ny)])
        with jax.named_scope("send_x"):
            ar_x[gx] = row
            for d in far_first:
                pltpu.make_async_remote_copy(ar_x.at[gx], ar_x.at[gx], a_send.at[1], a_recv.at[1],
                                             device_id=(wrapped(gx, d, nx), gy), device_id_type=MESH).start()
        with jax.named_scope("reduce_x"):
            all_send(ar_x, 1, nx - 1).wait_recv()
            row = tree_sum([ar_x[i] for i in range(nx)]) * scale
        with jax.named_scope("tail"):
            for step in range(STEPS):
                for i in range(2):
                    mom[step, i : i + 1, :] = roll(row, -LEVELS * (2 * step + i))[:, :LEVELS]
            for copy in copies:
                copy.wait_send()
            all_send(ar_y, 0, ny - 1).wait_send()
            all_send(ar_x, 1, nx - 1).wait_send()

    return kernel


def write_out(out_v, mom_v, out, mom, sem):
    first = pltpu.make_async_copy(out_v, out, sem.at[0])
    second = pltpu.make_async_copy(mom_v, mom, sem.at[1])
    first.start()
    second.start()
    first.wait()
    second.wait()


def shards(nx, ny, z_ring):
    def rows(x):
        a, b, cols, flat = x.shape
        x = x.reshape(a, b, cols, CHUNKS, 128).transpose(0, 1, 3, 2, 4)
        return x.reshape(a * b * CHUNKS * cols, 128)

    def step(droplets, moves, pairing, collisions):
        f32 = jnp.float32
        i32 = jnp.int32
        dma = pltpu.SemaphoreType.DMA
        hbm = pl.BlockSpec(memory_space=pl.ANY)
        vmem = pl.BlockSpec(memory_space=pltpu.VMEM)
        faces = pltpu.VMEM((STEPS, 2, 2, CHUNKS, SLOTS, 128), f32)
        pairs = (2, 2, CHUNKS, SLOTS, 128)
        n_known = len(doublings(nx)) + len(doublings(ny))
        out, mom = pl.pallas_call(
            make_kernel(nx, ny, z_ring),
            out_shape=(pltpu.VMEM((512, 128), f32), pltpu.VMEM((STEPS, 2, LEVELS), f32)),
            in_specs=[hbm] * 4,
            out_specs=(vmem, vmem),
            scratch_shapes=[
                pltpu.VMEM((512, 128), f32),
                pltpu.VMEM((512, 128), i32),
                pltpu.VMEM((512, 128), i32),
                pltpu.VMEM((256, 128), i32),
                pltpu.VMEM(pairs, f32),
                faces,
                faces,
                faces,
                pltpu.VMEM((STEPS, 2, 4, 8, 128), f32),
                pltpu.VMEM((STEPS, 2, 6, 8, 128), f32),
                pltpu.VMEM(pairs, i32),
                pltpu.VMEM(pairs, f32),
                pltpu.VMEM((ny, 1, 128), f32),
                pltpu.VMEM((nx, 1, 128), f32),
                dma((6,)),
                dma((STEPS, 2, 2, CHUNKS)),
                dma((STEPS, 2, 2, CHUNKS)),
                dma((STEPS, 2, 6)),
                dma((STEPS, 2, 6)),
                dma((2,)),
                dma((2,)),
                pltpu.SemaphoreType.REGULAR((max(n_known, 1),)),
            ],
            compiler_params=pltpu.CompilerParams(collective_id=0, has_side_effects=True),
        )(rows(droplets), rows(moves), rows(pairing), rows(collisions))
        out, mom = pl.pallas_call(
            write_out,
            out_shape=(jax.ShapeDtypeStruct((512, 128), f32), jax.ShapeDtypeStruct((STEPS, 2, LEVELS), f32)),
            in_specs=[vmem, vmem],
            out_specs=(hbm, hbm),
            scratch_shapes=[dma((2,))],
        )(pltpu.with_memory_space_constraint(out, pltpu.VMEM), pltpu.with_memory_space_constraint(mom, pltpu.VMEM))
        out = out.reshape(2, SLOTS, CHUNKS, 2, 128).transpose(0, 1, 3, 2, 4).reshape(droplets.shape)
        return out, mom

    return step


def solution(mesh, z_ring=Z_RING):
    placed = P(None, None, "gx", "gy")
    return jax.shard_map(
        shards(mesh.shape["gx"], mesh.shape["gy"], z_ring), mesh=mesh, in_specs=(placed,) * 4, out_specs=(placed, P()),
        check_vma=False,
    )
```

```python
import jax
import jax.numpy as jnp
from jax import lax
from jax.experimental import pallas as pl
from jax.experimental.pallas import tpu as pltpu
from jax.sharding import PartitionSpec as P

MESH = pl.DeviceIdType.MESH
SLOTS = 32
PAIRS = 16
LEVELS = 16
GROUPS = 4
CHUNKS = 4
STEPS = 2
Z_RING = 8
ORDER = (0, 3, 1, 2)
count_unit = 4096.0


def rim(step, nm):
    return 6 * nm if step == 0 else 12 + 10 * nm


def row0(base, slot, chunk, col):
    return ((base * SLOTS + slot) * CHUNKS + chunk) * 2 + col


def eight(base, group, chunk, col):
    return pl.ds(row0(base, 8 * group, chunk, col), 8, stride=8)


def roll(x, shift):
    return pltpu.roll(x, shift % 128, axis=x.ndim - 1)


def wrapped(i, d, size):
    j = i + d
    if d > 0:
        return jnp.where(j >= size, j - size, j)
    return jnp.where(j < 0, j + size, j)


def tree_sum(terms):
    while len(terms) > 1:
        terms = [a + b for a, b in zip(terms[::2], terms[1::2])] + ([terms[-1]] if len(terms) % 2 else [])
    return terms[0]


def doublings(size):
    return [1 << i for i in range(10) if (1 << i) < size // 2]


def make_kernel(nx, ny, z_ring):
    y_ring = nx // z_ring
    along_x = [z_ring * d for d in doublings(y_ring)] + doublings(z_ring)
    along_y = doublings(ny)
    scale = 1.0 / (nx * 2 * ny * 32 * count_unit)

    def hops(d):
        dy, dz = d // z_ring, d % z_ring
        return min(dy, y_ring - dy) + min(dz, z_ring - dz)

    far_first = sorted(range(1, nx), key=lambda d: -hops(d))

    def kernel(drop, mov, pair, coll, out, mom, d_in, m_in, p_in, c_in, st, fs, fr, own, rs, rr, code, coef, ar_y, ar_x,
               in_sem, send_sem, f_recv, r_recv, a_recv, known):
        gx = lax.axis_index("gx")
        gy = lax.axis_index("gy")
        halves = lambda src, dst, i, n: (src.at[pl.ds(i * n, n)], dst.at[pl.ds(i * n, n)])
        n_load, move_load, m_load, pair_load, coll_load, later_load = [
            pltpu.make_async_copy(src, dst, in_sem.at[i])
            for i, (src, dst) in enumerate(
                (
                    halves(drop, d_in, 0, 256),
                    halves(mov, m_in, 0, 256),
                    halves(drop, d_in, 1, 256),
                    (pair, p_in),
                    (coll, c_in),
                    halves(mov, m_in, 1, 256),
                )
            )
        ]
        n_load.start()
        move_load.start()
        xs = {0: gx, 1: wrapped(gx, 1, nx), -1: wrapped(gx, -1, nx)}
        ys = {0: gy, 1: wrapped(gy, 1, ny), -1: wrapped(gy, -1, ny)}
        barrier = pltpu.get_barrier_semaphore()
        greeted = [(xs[dx], ys[dy]) for dx, dy in ((-1, -1), (-1, 1), (1, -1), (1, 1), (-1, 0), (1, 0), (0, -1), (0, 1))]
        greeted += [(wrapped(gx, z_ring, nx), gy), (wrapped(gx, -z_ring, nx), gy)]
        for target in greeted:
            pl.semaphore_signal(barrier, inc=1, device_id=target, device_id_type=MESH)
        m_load.start()
        pair_load.start()
        coll_load.start()
        later_load.start()

        lane = lax.broadcasted_iota(jnp.int32, (8, 128), 1)
        first_row = lane < LEVELS
        last_row = lane >= 128 - LEVELS
        zero = jnp.zeros((8, 128), jnp.float32)

        def tell(i):
            targets = []
            if i < len(along_x):
                targets += [(wrapped(gx, e * along_x[i], nx), gy) for e in (1, -1)]
            if i < len(along_y):
                targets += [(gx, wrapped(gy, e * along_y[i], ny)) for e in (1, -1)]
            for target in targets:
                pl.semaphore_signal(known.at[i], inc=1, device_id=target, device_id_type=MESH)

        def hear(i):
            heard = 2 * (i < len(along_x)) + 2 * (i < len(along_y))
            if heard:
                pl.semaphore_wait(known.at[i], heard)

        def value(step, nm, col, k, g):
            if step == 0:
                return d_in[eight(nm, g, k, col), :]
            return st[nm, col, k, 8 * g : 8 * g + 8, :]

        def moves(step, col, k, g):
            return m_in[eight(step, g, k, col), :]

        def leaving(step, nm, side, k, g):
            x = value(step, nm, 1 - side, k, g)
            c = moves(step, 1 - side, k, g)
            first = 6 if side == 0 else 0
            return [jnp.where(c == first + i, x, zero) for i in range(3)]

        def staying(step, nm, col, k, g):
            x0 = value(step, nm, 0, k, g)
            x1 = value(step, nm, 1, k, g)
            c0 = moves(step, 0, k, g)
            c1 = moves(step, 1, k, g)
            a = 3 + 3 * col
            b = 3 * col
            return [jnp.where(c0 == a + i, x0, jnp.where(c1 == b + i, x1, zero)) for i in range(3)]

        def remote(src, dst, send, recv, target):
            pltpu.make_async_remote_copy(src, dst, send_sem.at[send], recv, device_id=target, device_id_type=MESH).start()

        def send_rims(step, nm, down):
            for kind, part in enumerate((staying, leaving)):
                pieces = []
                for i in range(2):
                    for g in range(GROUPS):
                        j = 16 * (i * GROUPS + g)
                        x = part(step, nm, i, 0 if down else CHUNKS - 1, g)[0 if down else 2]
                        pieces.append(jnp.where((lane >= j) & (lane < j + 16), roll(x, j if down else j + 16), zero))
                rs[step, nm, 2 * kind + down] = tree_sum(pieces)
                for side in range(kind + 1):
                    target = (xs[1 - 2 * side if kind else 0], ys[1 - 2 * down])
                    remote(rs.at[step, nm, 2 * kind + down], rr.at[rim(step, nm) + 2 * (kind + side) + down], 1, r_recv.at[step, nm],
                           target)

        def face_sem(step, nm, k):
            return f_recv.at[nm * CHUNKS + k if step == 0 else 2 * CHUNKS + nm]

        def send_face(step, nm, k):
            for side in range(2):
                remote(fs.at[step, nm, k, side], fr.at[step, nm, k, side], 0, face_sem(step, nm, k), (xs[1 - 2 * side], gy))

        def send_faces(nm, then):
            parts = {}

            def get(side, g, k):
                if (side, g, k) not in parts:
                    down, stay, up = leaving(0, nm, side, k, g)
                    parts[side, g, k] = (roll(down, -LEVELS), stay, roll(up, LEVELS))
                return parts[side, g, k]

            for k in ORDER:
                for side in range(2):
                    for g in range(GROUPS):
                        down, stay, up = get(side, g, k)
                        before = get(side, g, k - 1)[2] if k > 0 else zero
                        after = get(side, g, k + 1)[0] if k < CHUNKS - 1 else zero
                        fs[0, nm, k, side, 8 * g : 8 * g + 8, :] = (
                            stay + jnp.where(first_row, before, up) + jnp.where(last_row, after, down)
                        )
                send_face(0, nm, k)
                if k == ORDER[0]:
                    then()

        def send_part(nm, k, held):
            patches = []
            for side in range(2):
                pieces = []
                for g in range(GROUPS):
                    down, stay, up = leaving(1, nm, side, k, g)
                    down_r = roll(down, -LEVELS)
                    up_r = roll(up, LEVELS)
                    before = held[side, g, k - 1][2] if (side, g, k - 1) in held else zero
                    after = held[side, g, k + 1][0] if (side, g, k + 1) in held else zero
                    held[side, g, k] = (down_r, stay, up_r)
                    fs[1, nm, k, side, 8 * g : 8 * g + 8, :] = (
                        stay + jnp.where(first_row, before, up_r) + jnp.where(last_row, after, down_r)
                    )
                    if k in (1, 2):
                        j = 16 * g
                        pieces.append(jnp.where((lane >= j) & (lane < j + 16), roll(down, j), zero))
                    if k == 2:
                        j = 64 + 16 * g
                        pieces.append(jnp.where((lane >= j) & (lane < j + 16), roll(up, j + 16), zero))
                if pieces:
                    patches.append(tree_sum(pieces))
            send_face(1, nm, k)
            for side, patch in enumerate(patches):
                i = 2 * (k - 1) + side
                rs[1, nm, 4 + i] = patch
                remote(rs.at[1, nm, 4 + i], rr.at[rim(1, nm) + 6 + i], 1, r_recv.at[1, nm], (xs[1 - 2 * side], gy))

        def keep_own(step, nm):
            for col in range(2):
                for g in range(GROUPS):
                    downs, stays, ups = zip(*[staying(step, nm, col, k, g) for k in range(CHUNKS)])
                    ups = [zero] + [roll(x, LEVELS) for x in ups]
                    downs = [roll(x, -LEVELS) for x in downs] + [zero]
                    for k in range(CHUNKS):
                        own[step, nm, col, k, 8 * g : 8 * g + 8, :] = (
                            stays[k] + jnp.where(first_row, ups[k], ups[k + 1]) + jnp.where(last_row, downs[k + 1], downs[k])
                        )

        def arrived(buf, sem):
            pltpu.make_async_remote_copy(buf, buf, send_sem.at[0], sem, device_id=(gx, ys[1]), device_id_type=MESH).wait_recv()

        def wait_rims(step, nm):
            arrived(rr.at[pl.ds(rim(step, nm), 6 if step == 0 else 10)], r_recv.at[step, nm])
            low = rr[rim(step, nm) + 0] + jnp.where(lane < 64, rr[rim(step, nm) + 2], rr[rim(step, nm) + 4])
            high = rr[rim(step, nm) + 1] + jnp.where(lane < 64, rr[rim(step, nm) + 3], rr[rim(step, nm) + 5])
            return low, high

        def joined(step, nm, col, k, rims):
            parts = []
            for g in range(GROUPS):
                x = own[step, nm, col, k, 8 * g : 8 * g + 8, :] + fr[step, nm, k, col, 8 * g : 8 * g + 8, :]
                j = 16 * (col * GROUPS + g)
                if k == 0:
                    x = x + jnp.where(first_row, roll(rims[0], -j), zero)
                if k == CHUNKS - 1:
                    x = x + jnp.where(last_row, roll(rims[1], 112 - j), zero)
                if step > 0 and k < 2:
                    x = x + jnp.where(last_row, roll(rr[rim(step, nm) + 6 + 2 * k + col], 112 - 16 * g), zero)
                if step > 0 and k == 3:
                    x = x + jnp.where(first_row, roll(rr[rim(step, nm) + 8 + col], -64 - 16 * g), zero)
                parts.append(x)
            return parts

        def partner_of(parts, c):
            low = c & 7
            high = (c >> 3) & 3
            got = jnp.take_along_axis(parts[0], low, axis=0, mode="promise_in_bounds")
            for g in range(1, GROUPS):
                got = jnp.where(high == g, jnp.take_along_axis(parts[g], low, axis=0, mode="promise_in_bounds"), got)
            return got

        def pair_codes(step):
            def body(i, carry):
                col = i % 2
                k = i // 2
                slot = [lax.broadcasted_iota(jnp.int32, (8, 128), 0) + 8 * g for g in range(GROUPS)]
                acc = [jnp.zeros((8, 128), jnp.int32) for g in range(GROUPS)]
                for p in range(PAIRS):
                    a = jnp.broadcast_to(p_in[pl.ds(row0(step, 2 * p, k, col), 1), :], (8, 128))
                    b = jnp.broadcast_to(p_in[pl.ds(row0(step, 2 * p + 1, k, col), 1), :], (8, 128))
                    g0 = jnp.broadcast_to(c_in[pl.ds(((step * PAIRS + p) * CHUNKS + k) * 2 + col, 1), :], (8, 128)) * 32
                    for_a = b + g0 + 128
                    for_b = a + g0
                    for g in range(GROUPS):
                        acc[g] = jnp.where(a == slot[g], for_a, jnp.where(b == slot[g], for_b, acc[g]))
                for g in range(GROUPS):
                    code[step, col, k, 8 * g : 8 * g + 8, :] = acc[g]
                return carry

            lax.fori_loop(0, 2 * CHUNKS, body, 0)

        def coalesce_n(step, k, rims):
            total = []
            for col in range(2):
                parts = joined(step, 0, col, k, rims)
                for g in range(GROUPS):
                    c = code[step, col, k, 8 * g : 8 * g + 8, :]
                    mine = parts[g]
                    other = partner_of(parts, c)
                    g0 = ((c >> 5) & 3).astype(jnp.float32)
                    ahead = jnp.where(c >= 128, 0.5, 0.0)
                    big = jnp.maximum(mine, other)
                    small = jnp.minimum(mine, other)
                    mine_big = mine + ahead > other
                    fits = jnp.where(small * 3.0 <= big, 3.0, jnp.where(small * 2.0 <= big, 2.0, 1.0))
                    taken = jnp.minimum(g0, fits)
                    rest = big - taken * small
                    splits = rest == 0.0
                    half = jnp.floor(small * 0.5)
                    new = jnp.where(mine_big, jnp.where(splits, half, rest), jnp.where(splits, small - half, small))
                    coef[0, col, k, 8 * g : 8 * g + 8, :] = jnp.where(mine_big, jnp.where(splits, taken, 1.0), 1.0)
                    coef[1, col, k, 8 * g : 8 * g + 8, :] = jnp.where(mine_big, jnp.where(splits, 1.0, 0.0), taken)
                    st[0, col, k, 8 * g : 8 * g + 8, :] = new
                    total.append(new)
                    if step == STEPS - 1:
                        out[eight(0, g, k, col), :] = new
            return tree_sum(total)

        def coalesce_m(step, k, rims):
            total = []
            for col in range(2):
                parts = joined(step, 1, col, k, rims)
                for g in range(GROUPS):
                    c = code[step, col, k, 8 * g : 8 * g + 8, :]
                    other = partner_of(parts, c)
                    new = coef[0, col, k, 8 * g : 8 * g + 8, :] * parts[g] + coef[1, col, k, 8 * g : 8 * g + 8, :] * other
                    if step < STEPS - 1:
                        st[1, col, k, 8 * g : 8 * g + 8, :] = new
                    else:
                        out[eight(1, g, k, col), :] = new
                    total.append(st[0, col, k, 8 * g : 8 * g + 8, :] * new)
            return tree_sum(total)

        def fold(x):
            x = jnp.sum(x, axis=0, keepdims=True)
            return tree_sum([x] + [roll(x, LEVELS * d) for d in range(1, 128 // LEVELS)])

        slot = lane[:1] >> 4
        row = jnp.zeros((1, 128), jnp.float32)
        with jax.named_scope("load"):
            n_load.wait()
            move_load.wait()
        with jax.named_scope("barrier"):
            pl.semaphore_wait(barrier, len(greeted))
        for nm in range(2):
            with jax.named_scope("send"):
                if nm == 1:
                    m_load.wait()

                def both_rims(nm=nm):
                    for down in (1, 0):
                        send_rims(0, nm, down)
                    if nm == 0:
                        tell(0)

                send_faces(nm, both_rims)
        with jax.named_scope("own"):
            keep_own(0, 0)
            keep_own(0, 1)
        with jax.named_scope("codes"):
            pair_load.wait()
            coll_load.wait()
            later_load.wait()
            pair_codes(0)
        with jax.named_scope("round"):
            hear(0)
            tell(1)
        for nm, coalesce in enumerate((coalesce_n, coalesce_m)):
            with jax.named_scope("wait_rims"):
                rims = wait_rims(0, nm)
            held = {}
            sums = []
            for k in ORDER:
                with jax.named_scope("wait_face"):
                    arrived(fr.at[0, nm, k], face_sem(0, nm, k))
                with jax.named_scope("step"):
                    sums.append(coalesce(0, k, rims))
                    send_part(nm, k, held)
                    if k in (0, CHUNKS - 1):
                        send_rims(1, nm, int(k == 0))
            row = jnp.where(slot == nm, fold(tree_sum(sums)), row)
            if nm == 0:
                with jax.named_scope("round"):
                    hear(1)
                    tell(2)
        with jax.named_scope("own"):
            keep_own(1, 0)
            keep_own(1, 1)
        with jax.named_scope("codes"):
            pair_codes(1)
        for nm, coalesce in enumerate((coalesce_n, coalesce_m)):
            with jax.named_scope("wait_last"):
                arrived(fr.at[1, nm], face_sem(1, nm, 0))
                rims = wait_rims(1, nm)
            with jax.named_scope("coalesce"):
                total = tree_sum([coalesce(1, k, rims) for k in range(CHUNKS)])
                row = jnp.where(slot == 2 + nm, fold(total), row)
            if nm == 0:
                with jax.named_scope("round"):
                    hear(2)
                    tell(3)
        with jax.named_scope("reduce_y"):
            ar_y[gy] = row
            for d in range(1, ny):
                remote(ar_y.at[gy], ar_y.at[gy], 2, a_recv.at[0], (gx, wrapped(gy, d, ny)))
            hear(3)
            arrived(ar_y.at[pl.ds(0, ny - 1)], a_recv.at[0])
            row = tree_sum([ar_y[i] for i in range(ny)])
        with jax.named_scope("send_x"):
            ar_x[gx] = row
            for d in far_first:
                remote(ar_x.at[gx], ar_x.at[gx], 3, a_recv.at[1], (wrapped(gx, d, nx), gy))
        with jax.named_scope("reduce_x"):
            arrived(ar_x.at[pl.ds(0, nx - 1)], a_recv.at[1])
            row = tree_sum([ar_x[i] for i in range(nx)]) * scale
        with jax.named_scope("tail"):
            for step in range(STEPS):
                for i in range(2):
                    mom[step, i : i + 1, :] = roll(row, -LEVELS * (2 * step + i))[:, :LEVELS]
            for i, sent in enumerate((fs, rr, ar_y.at[pl.ds(0, ny - 1)], ar_x.at[pl.ds(0, nx - 1)])):
                pltpu.make_async_remote_copy(sent, sent, send_sem.at[i], f_recv.at[0], device_id=(gx, ys[1]),
                                             device_id_type=MESH).wait_send()

    return kernel


def write_out(out_v, mom_v, out, mom, sem):
    first = pltpu.make_async_copy(out_v, out, sem.at[0])
    second = pltpu.make_async_copy(mom_v, mom, sem.at[1])
    first.start()
    second.start()
    first.wait()
    second.wait()


def shards(nx, ny, z_ring):
    def rows(x):
        a, b, cols, flat = x.shape
        x = x.reshape(a, b, cols, CHUNKS, 128).transpose(0, 1, 3, 2, 4)
        return x.reshape(a * b * CHUNKS * cols, 128)

    def step(droplets, moves, pairing, collisions):
        f32 = jnp.float32
        i32 = jnp.int32
        dma = pltpu.SemaphoreType.DMA
        hbm = pl.BlockSpec(memory_space=pl.ANY)
        vmem = pl.BlockSpec(memory_space=pltpu.VMEM)
        faces = pltpu.VMEM((STEPS, 2, CHUNKS, 2, SLOTS, 128), f32)
        kept = pltpu.VMEM((STEPS, 2, 2, CHUNKS, SLOTS, 128), f32)
        pairs = (2, 2, CHUNKS, SLOTS, 128)
        out, mom = pl.pallas_call(
            make_kernel(nx, ny, z_ring),
            out_shape=(pltpu.VMEM((512, 128), f32), pltpu.VMEM((STEPS, 2, LEVELS), f32)),
            in_specs=[hbm] * 4,
            out_specs=(vmem, vmem),
            scratch_shapes=[
                pltpu.VMEM((512, 128), f32),
                pltpu.VMEM((512, 128), i32),
                pltpu.VMEM((512, 128), i32),
                pltpu.VMEM((256, 128), i32),
                pltpu.VMEM(pairs, f32),
                faces,
                faces,
                kept,
                pltpu.VMEM((STEPS, 2, 8, 8, 128), f32),
                pltpu.VMEM((32, 8, 128), f32),
                pltpu.VMEM(pairs, i32),
                pltpu.VMEM(pairs, f32),
                pltpu.VMEM((ny, 1, 128), f32),
                pltpu.VMEM((nx, 1, 128), f32),
                dma((6,)),
                dma((4,)),
                dma((2 * CHUNKS + 2,)),
                dma((STEPS, 2)),
                dma((2,)),
                pltpu.SemaphoreType.REGULAR((4,)),
            ],
            compiler_params=pltpu.CompilerParams(collective_id=0, has_side_effects=True),
        )(rows(droplets), rows(moves), rows(pairing), rows(collisions))
        out, mom = pl.pallas_call(
            write_out,
            out_shape=(jax.ShapeDtypeStruct((512, 128), f32), jax.ShapeDtypeStruct((STEPS, 2, LEVELS), f32)),
            in_specs=[vmem, vmem],
            out_specs=(hbm, hbm),
            scratch_shapes=[dma((2,))],
        )(pltpu.with_memory_space_constraint(out, pltpu.VMEM), pltpu.with_memory_space_constraint(mom, pltpu.VMEM))
        out = out.reshape(2, SLOTS, CHUNKS, 2, 128).transpose(0, 1, 3, 2, 4).reshape(droplets.shape)
        return out, mom

    return step


def solution(mesh, z_ring=Z_RING):
    placed = P(None, None, "gx", "gy")
    return jax.shard_map(
        shards(mesh.shape["gx"], mesh.shape["gy"], z_ring), mesh=mesh, in_specs=(placed,) * 4, out_specs=(placed, P()),
        check_vma=False,
    )
```
